256 devices in a mesh: task: 4 (over z_lo), tile: 64 (over y, z_hi, x, core).
Axes of the slice: x: 4, y: 4, z: 8 (z_hi: 2, z_lo: 4; z = z_hi * 4 + z_lo), core: 2. Of those that a mesh axis runs over, the one named last changes fastest.
Arguments:
- adjusted: bfloat16 [8, 3584, 18944], P('task', 'tile'), may hold values from -6 to 6
- fisher: bfloat16 [8, 3584, 18944], P('task', 'tile'), may hold values from 0.0099487305 to 10
Outputs:
- merged: bfloat16 [3584, 18944], P(None, ('task', 'tile'))
The draws below stay inside these ranges and needn't reach their ends.
All inputs are finite; a program needn't handle non-finite values.
Results may differ from the reference program's by a relative error of at most 0.001.
Values may be sent and summed in bfloat16 or wider, within the bound.
A program may use at most 64 MiB of HBM per device.

```python
import math
import jax
import jax.numpy as jnp
from jax import lax

D = 3584
FF = 18944
MODELS = 8


def level_of(own_key, extent, cuts, least, top_value):
    def one(position, shards_of):
        steps = jax.random.uniform(jax.random.fold_in(jax.random.fold_in(own_key, 6), position), (shards_of,), jnp.float32, least / len(cuts), top_value / len(cuts))
        return jnp.repeat(jnp.exp(steps), extent[position] // shards_of).reshape((-1,) + (1,) * (len(extent) - position - 1))

    factor_of = one(*cuts[0])
    for cut in cuts[1:]:
        factor_of = factor_of * one(*cut)
    return factor_of


def gaussian(stream_key, dims, width, most, shards=(), dtype=jnp.bfloat16):
    array = width * jax.random.normal(stream_key, dims, jnp.float32)
    if shards:
        array = array * level_of(stream_key, dims, shards, -0.22, 0.18)
    return jnp.clip(array, -most, most).astype(dtype)


def setup_inputs(seed: int = 0) -> dict:
    keys = jax.random.split(jax.random.key(seed), 3)
    adjusted = gaussian(keys[0], (MODELS, D, FF), 1.0, 6.0, ((0, 4), (1, 64)))
    fisher = jnp.clip(jnp.exp(math.log(10.0) - 6.912895 * jax.random.uniform(keys[1], (MODELS, D, FF), jnp.float32) ** level_of(keys[1], (MODELS, D, FF), ((0, 4), (1, 64)), -0.2, 0.2)), 0.0099487305, 10.0).astype(jnp.bfloat16)
    return dict(adjusted=adjusted, fisher=fisher)


def reference(adjusted, fisher):
    def accumulate(carry, pair):
        numerator, denominator = carry
        weights, curvature = pair
        scaled = curvature.astype(jnp.float32)
        return (numerator + scaled * weights.astype(jnp.float32), denominator + scaled), None

    zeros = jnp.zeros((D, FF), jnp.float32)
    (numerator, denominator), unused = lax.scan(accumulate, (zeros, zeros), (adjusted, fisher))
    return (numerator / denominator).astype(jnp.bfloat16)
```

```python
import functools
import math

import jax
import jax.numpy as jnp
from jax import lax
from jax.experimental import pallas as pl
from jax.experimental.pallas import tpu as pltpu
from jax.sharding import PartitionSpec as P

MESH = pl.DeviceIdType.MESH
F32 = jnp.float32
BF16 = jnp.bfloat16

ROWS, TILES, LANES = 7, 37, 128
QUARTER = TILES * LANES
SEG, SEG_PAD, OWN = 592, 640, 74
PIECES = ((0, 19), (19, 18))
GROUP = 5
STEPS = 2 * ROWS
AHEAD, LAG, SKEW = 5, 3, 2

Q_POWER, Q_TOP, Q_KNEE = 24.0, 120.0, -9.5
Q_FLOOR = 2.0 ** (Q_TOP + Q_POWER * Q_KNEE)
Q_LINE = Q_FLOOR / 2.0**Q_KNEE
D_POWER, D_MID = 25.0, -1.665
INV_LN2 = 1.0 / math.log(2.0)


def log2(x):
    return jnp.log(x) * INV_LN2


def encode_q(q, inverse_scale):
    y = jnp.abs(q) * inverse_scale
    knee = 2.0**Q_KNEE
    power = jnp.exp2(log2(jnp.maximum(y, knee)) * Q_POWER + Q_TOP)
    code = jnp.where(y >= knee, power, y * Q_LINE)
    return jnp.where(q < 0, -code, code).astype(BF16)


def decode_q(code, scale):
    c = code.astype(F32)
    size = jnp.abs(c)
    root = jnp.exp2((log2(jnp.maximum(size, Q_FLOOR)) - Q_TOP) * (1.0 / Q_POWER))
    y = jnp.where(size >= Q_FLOOR, root, size * (1.0 / Q_LINE)) * scale
    return jnp.where(c < 0, -y, y)


def encode_d(d, log_count):
    return jnp.exp2((log2(d) - (log_count + D_MID)) * D_POWER).astype(BF16)


def decode_d(code, log_count):
    return jnp.exp2(log2(code.astype(F32)) * (1.0 / D_POWER) + (log_count + D_MID))


def lanes(tile, count=1):
    start = tile * LANES
    return pl.ds(start if isinstance(start, int) else pl.multiple_of(start, LANES), count * LANES)


def groups(start, count):
    return [range(a, min(a + GROUP, start + count)) for a in range(start, start + count, GROUP)]


def kernel(a_hbm, f_hbm, out, av, fv, up_in, up_out, dn_in, dn_out, merged, seg_out, seg_in, split,
           in_sem, chain_recv, chain_send, seg_recv, seg_send, out_recv, out_send):
    task, tile = lax.axis_index("task"), lax.axis_index("tile")
    slot, side = tile // 8, tile % 8

    def loads(r):
        return (pltpu.make_async_copy(a_hbm.at[:, r], av.at[:, r], in_sem.at[0, r]),
                pltpu.make_async_copy(f_hbm.at[:, r], fv.at[:, r], in_sem.at[1, r]))

    for r in range(ROWS):
        for copy in loads(r):
            copy.start()

    barrier = pltpu.get_barrier_semaphore()
    place = task * 8 + slot

    def greet_column(i, carry):
        other = (place + i) % 32
        pl.semaphore_signal(barrier, inc=1, device_id=(other // 8, (other % 8) * 8 + side), device_id_type=MESH)
        return carry

    def greet_side(i, carry):
        pl.semaphore_signal(barrier, inc=1, device_id=(task, slot * 8 + (side + i) % 8), device_id_type=MESH)
        return carry

    lax.fori_loop(1, 32, greet_column, 0)
    lax.fori_loop(1, 8, greet_side, 0)
    pl.semaphore_wait(barrier, 38)

    def wait_rows(i):
        @pl.when(i % 2 == 0)
        def _():
            for copy in loads(i // 2):
                copy.wait()

    def own(i, first_task, tiles):
        r, t = i // 2, i % 2
        base = (first_task + t) * TILES
        n, d = [], []
        for x in tiles:
            at = lanes(base + x)
            f0, f1 = fv[0, r, :, at].astype(F32), fv[1, r, :, at].astype(F32)
            n.append(f0 * av[0, r, :, at].astype(F32) + f1 * av[1, r, :, at].astype(F32))
            d.append(f0 + f1)
        return n, d

    def own_scale(i, first_task):
        r, t = i // 2, i % 2
        base = (first_task + t) * TILES
        tops = [jnp.full((8, LANES), 2.0**-96, F32) for _ in range(4)]
        for x in range(TILES):
            at = lanes(base + x)
            for m in range(2):
                k = (2 * x + m) % 4
                tops[k] = jnp.maximum(tops[k], jnp.abs(av[m, r, :, at].astype(F32)))
        return jnp.maximum(jnp.maximum(tops[0], tops[1]), jnp.maximum(tops[2], tops[3]))

    def span(piece):
        start, count = PIECES[piece]
        low = 0 if piece == 0 else 1 + 2 * start
        return pl.ds(low * LANES, (1 + 2 * (start + count) - low) * LANES)

    def hop(i, piece, source, target, way, to):
        r, t = i // 2, i % 2
        at = span(piece)
        return pltpu.make_async_remote_copy(
            src_ref=source.at[r, t, :, at], dst_ref=target.at[r, t, :, at],
            send_sem=chain_send.at[way], recv_sem=chain_recv.at[way, i, piece],
            device_id=(to, tile), device_id_type=MESH)

    def arrived(i, piece, target, way):
        r, t = i // 2, i % 2
        at = span(piece)
        pltpu.make_async_copy(target.at[r, t, :, at], target.at[r, t, :, at], chain_recv.at[way, i, piece]).wait()

    def received(i, piece, tiles, source, log_count, scale):
        r, t = i // 2, i % 2
        start, count = PIECES[piece]
        q = [decode_q(source[r, t, :, lanes(1 + start + x)], scale) for x in tiles]
        d = [decode_d(source[r, t, :, lanes(1 + start + count + x)], log_count) for x in tiles]
        return q, d

    def put(i, piece, tiles, n, d, target, log_count, inverse):
        r, t = i // 2, i % 2
        start, count = PIECES[piece]
        q = [encode_q(a / b, inverse) for a, b in zip(n, d)]
        e = [encode_d(b, log_count) for b in d]
        for x, code in zip(tiles, q):
            target[r, t, :, lanes(1 + start + x)] = code
        for x, code in zip(tiles, e):
            target[r, t, :, lanes(1 + start + count + x)] = code

    def first(i, first_task, way, target, landing, to):
        wait_rows(i)
        scale = own_scale(i, first_task)
        inverse = 1.0 / scale
        target[i // 2, i % 2, :, lanes(0)] = scale.astype(BF16)
        for piece, (start, count) in enumerate(PIECES):
            for tiles in groups(start, count):
                n, d = own(i, first_task, tiles)
                put(i, piece, tiles, n, d, target, 1.0, inverse)
            hop(i, piece, target, landing, way, to).start()

    def middle(i, first_task, way, source, target, to, log_in, log_out, wait_for_rows):
        if wait_for_rows:
            wait_rows(i)
        mine = own_scale(i, first_task)
        for piece, (start, count) in enumerate(PIECES):
            arrived(i, piece, source, way)
            if piece == 0:
                before = source[i // 2, i % 2, :, lanes(0)].astype(F32)
                scale = jnp.maximum(before, mine)
                inverse = 1.0 / scale
                target[i // 2, i % 2, :, lanes(0)] = scale.astype(BF16)
            for tiles in groups(start, count):
                n, d = own(i, first_task, tiles)
                q, e = received(i, piece, tiles, source, log_in, before)
                n = [x + a * b for x, a, b in zip(n, q, e)]
                d = [x + b for x, b in zip(d, e)]
                put(i, piece, tiles, n, d, target, log_out, inverse)
            hop(i, piece, target, source, way, to).start()

    lane = lax.broadcasted_iota(jnp.int32, (8, LANES), 1)

    def last(i, first_task, way, source):
        r, t = i // 2, i % 2
        for piece, (start, count) in enumerate(PIECES):
            arrived(i, piece, source, way)
            if piece == 0:
                before = source[r, t, :, lanes(0)].astype(F32)
            for tiles in groups(start, count):
                n, d = own(i, first_task, tiles)
                q, e = received(i, piece, tiles, source, math.log2(6.0), before)
                for x, n1, d1, q1, e1 in zip(tiles, n, d, q, e):
                    merged[:, lanes(x)] = (n1 + q1 * e1) / (d1 + e1)
        for k in range(8):
            low, off = SEG * k // LANES, SEG * k % LANES
            parts = [merged[:, lanes(low + j)] for j in range(6 if off else 5)]
            if off:
                parts = [pltpu.roll(x, LANES - off, 1) for x in parts]
                parts = [jnp.where(lane < LANES - off, parts[j], parts[j + 1]) for j in range(5)]
            for j in range(5):
                seg_out[r, t, k, :, lanes(j)] = parts[j].astype(BF16)
        for k in range(8):
            pltpu.make_async_remote_copy(
                src_ref=seg_out.at[r, t, k], dst_ref=seg_in.at[r, slot],
                send_sem=seg_send, recv_sem=seg_recv.at[r],
                device_id=(first_task + t, k * 8 + side), device_id_type=MESH).start()

    lane3 = lax.broadcasted_iota(jnp.int32, (8, 8, LANES), 2)

    def spread(r):
        pltpu.make_async_copy(seg_in.at[r], seg_in.at[r], seg_recv.at[r]).wait()
        for k in range(8):
            low, off = OWN * k // LANES, OWN * k % LANES
            part = seg_in[r, :, :, lanes(low)].astype(F32)
            if off:
                part = pltpu.roll(part, LANES - off, 2)
            if off + OWN > LANES:
                more = pltpu.roll(seg_in[r, :, :, lanes(low + 1)].astype(F32), LANES - off, 2)
                part = jnp.where(lane3 < LANES - off, part, more)
            split[r, k] = part.astype(BF16)
        pltpu.make_async_copy(split.at[r, side], out.at[:, side, r], out_recv).start()

        def send(i, carry):
            k = (side + i) % 8
            pltpu.make_async_remote_copy(
                src_ref=split.at[r, k], dst_ref=out.at[:, side, r],
                send_sem=out_send, recv_sem=out_recv,
                device_id=(task, slot * 8 + k), device_id_type=MESH).start()
            return carry

        lax.fori_loop(1, 8, send, 0)

    def loop(low, high, body):
        def step(i, carry):
            body(i)
            return carry

        lax.fori_loop(low, high, step, 0)

    def outer(send_task, send_way, target, landing, to, merge_task, merge_way, source):
        def go(i):
            first(i, send_task, send_way, target, landing, to)

        loop(0, AHEAD, go)

        def step(i):
            last(i, merge_task, merge_way, source)

            @pl.when(i + AHEAD < STEPS)
            def _():
                go(i + AHEAD)

            @pl.when((i % 2 == 1) & (i // 2 >= LAG))
            def _():
                spread(i // 2 - LAG)

        loop(0, STEPS, step)
        loop(ROWS - LAG, ROWS, spread)

    def inner(lead, trail):
        def step(i):
            @pl.when(i < STEPS)
            def _():
                lead(i, True)

            @pl.when(i >= SKEW)
            def _():
                trail(i - SKEW, False)

            @pl.when((i % 2 == 1) & (i // 2 >= LAG))
            def _():
                spread(i // 2 - LAG)

        loop(0, STEPS + SKEW, step)
        loop((STEPS + SKEW) // 2 - LAG, ROWS, spread)

    log6 = math.log2(6.0)

    def up(log_in, log_out, to):
        return lambda i, rows: middle(i, 0, 0, up_in, up_out, to, log_in, log_out, rows)

    def down(log_in, log_out, to):
        return lambda i, rows: middle(i, 2, 1, dn_in, dn_out, to, log_in, log_out, rows)

    merged[:, lanes(TILES)] = jnp.zeros((8, LANES), F32)

    def whole(ref, sem):
        pltpu.make_async_copy(ref, ref, sem).wait()

    @pl.when(task == 0)
    def _():
        outer(0, 0, up_out, up_in, 1, 2, 1, dn_in)
        whole(up_out, chain_send.at[0])
        whole(seg_out, seg_send)

    @pl.when(task == 3)
    def _():
        outer(2, 1, dn_out, dn_in, 2, 0, 0, up_in)
        whole(dn_out, chain_send.at[1])
        whole(seg_out, seg_send)

    @pl.when(task == 1)
    def _():
        inner(up(1.0, 2.0, 2), down(2.0, log6, 0))
        whole(up_out, chain_send.at[0])
        whole(dn_out, chain_send.at[1])

    @pl.when(task == 2)
    def _():
        inner(down(1.0, 2.0, 1), up(2.0, log6, 3))
        whole(up_out, chain_send.at[0])
        whole(dn_out, chain_send.at[1])

    rest = split.at[:, pl.ds(0, 7)]
    whole(rest, out_send)
    whole(out, out_recv)


def body(adjusted, fisher):
    models, rows, columns = adjusted.shape
    shape = (models, ROWS, 8, columns)
    chain = pltpu.VMEM((ROWS, 2, 8, (1 + 2 * TILES) * LANES), BF16)
    out = pl.pallas_call(
        kernel,
        out_shape=jax.ShapeDtypeStruct((8, 8, ROWS, 8, LANES), BF16),
        in_specs=[pl.BlockSpec(memory_space=pl.ANY)] * 2,
        out_specs=pl.BlockSpec(memory_space=pltpu.VMEM),
        scratch_shapes=[
            pltpu.VMEM(shape, BF16),
            pltpu.VMEM(shape, BF16),
            chain, chain, chain, chain,
            pltpu.VMEM((8, (TILES + 1) * LANES), F32),
            pltpu.VMEM((ROWS, 2, 8, 8, SEG_PAD), BF16),
            pltpu.VMEM((ROWS, 8, 8, SEG_PAD), BF16),
            pltpu.VMEM((ROWS, 8, 8, 8, LANES), BF16),
            pltpu.SemaphoreType.DMA((2, ROWS)),
            pltpu.SemaphoreType.DMA((2, STEPS, len(PIECES))),
            pltpu.SemaphoreType.DMA((2,)),
            pltpu.SemaphoreType.DMA((ROWS,)),
            pltpu.SemaphoreType.DMA,
            pltpu.SemaphoreType.DMA,
            pltpu.SemaphoreType.DMA,
        ],
        compiler_params=pltpu.CompilerParams(collective_id=0, has_side_effects=True),
    )(adjusted.reshape(shape), fisher.reshape(shape))
    return out.reshape(-1, LANES)[:, :OWN]


def solution(mesh):
    return jax.shard_map(
        body,
        mesh=mesh,
        in_specs=(P("task", "tile", None), P("task", "tile", None)),
        out_specs=P(None, ("task", "tile")),
        check_vma=False,
    )
```

```python
import functools
import math

import jax
import jax.numpy as jnp
from jax import lax
from jax.experimental import pallas as pl
from jax.experimental.pallas import tpu as pltpu
from jax.sharding import PartitionSpec as P

MESH = pl.DeviceIdType.MESH
F32 = jnp.float32
BF16 = jnp.bfloat16

ROWS, TILES, LANES = 7, 37, 128
SEG, SEG_PAD, OWN = 592, 640, 74
PIECES = ((0, 10), (10, 9), (19, 9), (28, 9))
GROUP = 5
STEPS = 2 * ROWS
AHEAD, LAG, SKEW = 5, 3, 5
EVEN = (*range(0, 5), *range(9, 14), *range(18, 23), *range(28, 32))
ODD = (*range(5, 9), *range(14, 18), *range(23, 28), *range(32, 37))
HEAD = {1: 48, 3: 16, 4: 0, 6: 32}
TAIL = {1: 48, 3: 16, 4: 64, 6: 32}

Q_POWER, Q_TOP, Q_KNEE = 24.0, 120.0, -9.5
Q_FLOOR = 2.0 ** (Q_TOP + Q_POWER * Q_KNEE)
Q_LINE = Q_FLOOR / 2.0**Q_KNEE
D_POWER, D_MID = 25.0, -1.665
INV_LN2 = 1.0 / math.log(2.0)


def log2(x):
    return jnp.log(x) * INV_LN2


def encode_q(q, inverse_scale):
    y = jnp.abs(q) * inverse_scale
    knee = 2.0**Q_KNEE
    power = jnp.exp2(log2(jnp.maximum(y, knee)) * Q_POWER + Q_TOP)
    code = jnp.where(y >= knee, power, y * Q_LINE)
    return jnp.where(q < 0, -code, code).astype(BF16)


def decode_q(code, scale):
    c = code.astype(F32)
    size = jnp.abs(c)
    root = jnp.exp2((log2(jnp.maximum(size, Q_FLOOR)) - Q_TOP) * (1.0 / Q_POWER))
    y = jnp.where(size >= Q_FLOOR, root, size * (1.0 / Q_LINE)) * scale
    return jnp.where(c < 0, -y, y)


def encode_d(d, log_count):
    return jnp.exp2((log2(d) - (log_count + D_MID)) * D_POWER).astype(BF16)


def decode_d(code, log_count):
    return jnp.exp2(log2(code.astype(F32)) * (1.0 / D_POWER) + (log_count + D_MID))


def lanes(tile, count=1):
    start = tile * LANES
    return pl.ds(start if isinstance(start, int) else pl.multiple_of(start, LANES), count * LANES)


def groups(start, count):
    return [range(a, min(a + GROUP, start + count)) for a in range(start, start + count, GROUP)]


def kernel(a_hbm, f_hbm, out, av, fv, up_in, up_out, dn_in, dn_out, merged, seg_out, seg_in, edge_out, edge_in, split,
           in_sem, chain_recv, chain_send, seg_recv, seg_send, edge_recv, edge_send, out_recv, out_send):
    task, tile = lax.axis_index("task"), lax.axis_index("tile")
    slot, side = tile // 8, tile % 8

    def loads(r):
        return (pltpu.make_async_copy(a_hbm.at[:, r], av.at[:, r], in_sem.at[0, r]),
                pltpu.make_async_copy(f_hbm.at[:, r], fv.at[:, r], in_sem.at[1, r]))

    for r in range(ROWS):
        for copy in loads(r):
            copy.start()

    edge_in[...] = jnp.zeros_like(edge_in)
    barrier = pltpu.get_barrier_semaphore()
    place = task * 8 + slot

    def greet_column(i, carry):
        other = (place + i) % 32
        pl.semaphore_signal(barrier, inc=1, device_id=(other // 8, (other % 8) * 8 + side), device_id_type=MESH)
        return carry

    def greet_side(i, carry):
        pl.semaphore_signal(barrier, inc=1, device_id=(task, slot * 8 + (side + i) % 8), device_id_type=MESH)
        return carry

    lax.fori_loop(1, 32, greet_column, 0)
    lax.fori_loop(1, 8, greet_side, 0)

    def wait_rows(i):
        @pl.when(i % 2 == 0)
        def _():
            for copy in loads(i // 2):
                copy.wait()

    half = slot % 2
    odd_task = (3 * half, 3 - 3 * half)
    even_task = (3 - 3 * half, 3 * half)

    def column(i, way, x):
        if x < len(ODD):
            other = odd_task[way] * TILES + ODD[x]
        else:
            other = even_task[way] * TILES + EVEN[x - len(ODD)]
        return lanes(jnp.where(i % 2 == 0, (1 + way) * TILES + x, other))

    def own(i, way, tiles):
        r = i // 2
        n, d = [], []
        for x in tiles:
            at = column(i, way, x)
            f0, f1 = fv[0, r, :, at].astype(F32), fv[1, r, :, at].astype(F32)
            n.append(f0 * av[0, r, :, at].astype(F32) + f1 * av[1, r, :, at].astype(F32))
            d.append(f0 + f1)
        return n, d

    def own_scale(i, way):
        r = i // 2
        tops = [jnp.full((8, LANES), 2.0**-96, F32) for _ in range(4)]
        for x in range(TILES):
            at = column(i, way, x)
            for m in range(2):
                k = (2 * x + m) % 4
                tops[k] = jnp.maximum(tops[k], jnp.abs(av[m, r, :, at].astype(F32)))
        return jnp.maximum(jnp.maximum(tops[0], tops[1]), jnp.maximum(tops[2], tops[3]))

    def span(piece):
        start, count = PIECES[piece]
        low = 0 if piece == 0 else 1 + 2 * start
        return pl.ds(low * LANES, (1 + 2 * (start + count) - low) * LANES)

    def hop(i, piece, source, target, way, to):
        r, t = i // 2, i % 2
        at = span(piece)
        return pltpu.make_async_remote_copy(
            src_ref=source.at[r, t, :, at], dst_ref=target.at[r, t, :, at],
            send_sem=chain_send.at[way], recv_sem=chain_recv.at[way, i, piece],
            device_id=(to, tile), device_id_type=MESH)

    def arrived(i, piece, target, way):
        r, t = i // 2, i % 2
        at = span(piece)
        pltpu.make_async_copy(target.at[r, t, :, at], target.at[r, t, :, at], chain_recv.at[way, i, piece]).wait()

    def received(i, piece, tiles, source, log_count, scale):
        r, t = i // 2, i % 2
        start, count = PIECES[piece]
        q = [decode_q(source[r, t, :, lanes(1 + start + x)], scale) for x in tiles]
        d = [decode_d(source[r, t, :, lanes(1 + start + count + x)], log_count) for x in tiles]
        return q, d

    def put(i, piece, tiles, n, d, target, log_count, inverse):
        r, t = i // 2, i % 2
        start, count = PIECES[piece]
        q = [encode_q(a / b, inverse) for a, b in zip(n, d)]
        e = [encode_d(b, log_count) for b in d]
        for x, code in zip(tiles, q):
            target[r, t, :, lanes(1 + start + x)] = code
        for x, code in zip(tiles, e):
            target[r, t, :, lanes(1 + start + count + x)] = code

    def first(i, way, target, landing, to, send=True):
        wait_rows(i)
        scale = own_scale(i, way)
        inverse = 1.0 / scale
        target[i // 2, i % 2, :, lanes(0)] = scale.astype(BF16)
        for piece, (start, count) in enumerate(PIECES):
            for tiles in groups(start, count):
                n, d = own(i, way, tiles)
                put(i, piece, tiles, n, d, target, 1.0, inverse)
            if send:
                hop(i, piece, target, landing, way, to).start()

    def middle(i, piece, way, source, target, to, log_in, log_out):
        r, t = i // 2, i % 2
        start, count = PIECES[piece]
        if piece == 0:
            mine = own_scale(i, way)
        arrived(i, piece, source, way)
        before = source[r, t, :, lanes(0)].astype(F32)
        if piece == 0:
            scale = jnp.maximum(before, mine)
            target[r, t, :, lanes(0)] = scale.astype(BF16)
        else:
            scale = target[r, t, :, lanes(0)].astype(F32)
        inverse = 1.0 / scale
        for tiles in groups(start, count):
            n, d = own(i, way, tiles)
            q, e = received(i, piece, tiles, source, log_in, before)
            n = [x + a * b for x, a, b in zip(n, q, e)]
            d = [x + b for x, b in zip(d, e)]
            put(i, piece, tiles, n, d, target, log_out, inverse)
        hop(i, piece, target, source, way, to).start()

    lane = lax.broadcasted_iota(jnp.int32, (8, LANES), 1)

    def last(i, way, source):
        r, t = i // 2, i % 2
        for piece, (start, count) in enumerate(PIECES):
            arrived(i, piece, source, way)
            if piece == 0:
                before = source[r, t, :, lanes(0)].astype(F32)
            for tiles in groups(start, count):
                n, d = own(i, way, tiles)
                q, e = received(i, piece, tiles, source, math.log2(6.0), before)
                for x, n1, d1, q1, e1 in zip(tiles, n, d, q, e):
                    merged[:, lanes(x)] = (n1 + q1 * e1) / (d1 + e1)

        def shift(where, k):
            part = merged[:, lanes(where)]
            return pltpu.roll(part, LANES - SEG * k % LANES, 1) if SEG * k % LANES else part

        def join(low, high, edge):
            if low is None or high is None:
                return high if low is None else low
            return jnp.where(lane < edge, low, high)

        def pack(place_of):
            for k in range(8):
                low, off = SEG * k // LANES, SEG * k % LANES
                held = [place_of(k, low + j) for j in range(6 if off else 5)]
                parts = [None if x is None else shift(x, k) for x in held]
                for j in range(5):
                    part = join(parts[j], parts[j + 1], LANES - off) if off else parts[j]
                    seg_out[r, 8 * t + k, :, lanes(j)] = part.astype(BF16)

        @pl.when(t == 0)
        def _():
            pack(lambda k, x: x if x < TILES else None)
            for k in range(8):
                pltpu.make_async_remote_copy(
                    src_ref=seg_out.at[r, k], dst_ref=seg_in.at[r, slot],
                    send_sem=seg_send, recv_sem=seg_recv.at[r],
                    device_id=(1 + way, k * 8 + side), device_id_type=MESH).start()

        @pl.when(t == 1)
        def _():
            def place_of(k, x):
                if k % 2:
                    return ODD.index(x) if x in ODD else None
                return len(ODD) + EVEN.index(x) if x in EVEN else None

            pack(place_of)
            for e, k in enumerate(sorted(HEAD)):
                first_tile, last_tile = SEG * k // LANES, (SEG * (k + 1) - 1) // LANES
                low = None if HEAD[k] == 0 else shift(place_of(k + 1, first_tile), k)
                edge_out[r, e] = join(low, shift(place_of(k + 1, last_tile), k), HEAD[k]).astype(BF16)
            for k in range(8):
                to = odd_task[way] if k % 2 else even_task[way]
                mine = (to == task) & (k == slot)

                @pl.when(mine)
                def _():
                    pltpu.make_async_copy(seg_out.at[r, 8 + k], seg_in.at[r, slot], seg_recv.at[r]).start()

                @pl.when(jnp.logical_not(mine))
                def _():
                    pltpu.make_async_remote_copy(
                        src_ref=seg_out.at[r, 8 + k], dst_ref=seg_in.at[r, slot],
                        send_sem=seg_send, recv_sem=seg_recv.at[r],
                        device_id=(to, k * 8 + side), device_id_type=MESH).start()
            for e, k in enumerate(sorted(HEAD)):
                to = even_task[way] if k % 2 else odd_task[way]
                pltpu.make_async_remote_copy(
                    src_ref=edge_out.at[r, e], dst_ref=edge_in.at[r, slot],
                    send_sem=edge_send, recv_sem=edge_recv.at[r],
                    device_id=(to, k * 8 + side), device_id_type=MESH).start()

    lane3 = lax.broadcasted_iota(jnp.int32, (8, 8, LANES), 2)

    shared = (task % 3 == 0) & ((slot % 5 == 1) | (slot == 3) | (slot == 4))
    head, tail = jnp.int32(0), jnp.int32(LANES)
    for k in HEAD:
        head = jnp.where(shared & (slot == k), HEAD[k], head)
        tail = jnp.where(shared & (slot == k), TAIL[k], tail)

    def spread(r):
        pltpu.make_async_copy(seg_in.at[r], seg_in.at[r], seg_recv.at[r]).wait()

        @pl.when(shared)
        def _():
            pltpu.make_async_copy(edge_in.at[r], edge_in.at[r], edge_recv.at[r]).wait()

        edge = edge_in[r].astype(F32)
        tiles = [seg_in[r, :, :, lanes(j)].astype(F32) for j in range(5)]
        tiles[0] = jnp.where(lane3 < head, edge, tiles[0])
        tiles[4] = jnp.where(lane3 >= tail, edge, tiles[4])
        for k in range(8):
            low, off = OWN * k // LANES, OWN * k % LANES
            part = tiles[low]
            if off:
                part = pltpu.roll(part, LANES - off, 2)
            if off + OWN > LANES:
                more = pltpu.roll(tiles[low + 1], LANES - off, 2)
                part = jnp.where(lane3 < LANES - off, part, more)
            split[r, k] = part.astype(BF16)
        pltpu.make_async_copy(split.at[r, side], out.at[:, side, r], out_recv).start()

        def send(i, carry):
            k = (side + i) % 8
            pltpu.make_async_remote_copy(
                src_ref=split.at[r, k], dst_ref=out.at[:, side, r],
                send_sem=out_send, recv_sem=out_recv,
                device_id=(task, slot * 8 + k), device_id_type=MESH).start()
            return carry

        lax.fori_loop(1, 8, send, 0)

    def loop(low, high, body):
        def step(i, carry):
            body(i)
            return carry

        lax.fori_loop(low, high, step, 0)

    def outer(send_way, target, landing, to, merge_way, source):
        def go(i):
            first(i, send_way, target, landing, to)

        for piece in range(len(PIECES)):
            hop(0, piece, target, landing, send_way, to).start()
        loop(1, AHEAD, go)

        def step(i):
            last(i, merge_way, source)

            @pl.when(i + AHEAD < STEPS)
            def _():
                go(i + AHEAD)

            @pl.when((i % 2 == 1) & (i // 2 >= LAG))
            def _():
                spread(i // 2 - LAG)

        loop(0, STEPS, step)
        loop(ROWS - LAG, ROWS, spread)

    def inner(lead, trail):
        def step(i):
            @pl.when(i < STEPS)
            def _():
                wait_rows(i)

            for piece in range(len(PIECES)):
                back, late = (piece - SKEW) // len(PIECES), (piece - SKEW) % len(PIECES)

                @pl.when(i < STEPS)
                def _():
                    lead(i, piece)

                @pl.when((i + back >= 0) & (i + back < STEPS))
                def _():
                    trail(i + back, late)

            @pl.when((i % 2 == 1) & (i // 2 >= LAG) & (i // 2 - LAG < ROWS))
            def _():
                spread(i // 2 - LAG)

        steps = STEPS - (-SKEW // len(PIECES))
        loop(0, steps, step)
        loop(max(steps // 2 - LAG, 0), ROWS, spread)

    log6 = math.log2(6.0)

    def up(log_in, log_out, to):
        return lambda i, piece: middle(i, piece, 0, up_in, up_out, to, log_in, log_out)

    def down(log_in, log_out, to):
        return lambda i, piece: middle(i, piece, 1, dn_in, dn_out, to, log_in, log_out)

    @pl.when(task == 0)
    def _():
        first(0, 0, up_out, up_in, 1, False)

    @pl.when(task == 3)
    def _():
        first(0, 1, dn_out, dn_in, 2, False)

    pl.semaphore_wait(barrier, 38)

    def whole(ref, sem):
        pltpu.make_async_copy(ref, ref, sem).wait()

    @pl.when(task == 0)
    def _():
        outer(0, up_out, up_in, 1, 1, dn_in)
        whole(up_out, chain_send.at[0])
        whole(seg_out.at[:, pl.ds(0, 15)], seg_send)
        whole(edge_out, edge_send)

    @pl.when(task == 3)
    def _():
        outer(1, dn_out, dn_in, 2, 0, up_in)
        whole(dn_out, chain_send.at[1])
        whole(seg_out.at[:, pl.ds(0, 15)], seg_send)
        whole(edge_out, edge_send)

    @pl.when(task == 1)
    def _():
        inner(up(1.0, 2.0, 2), down(2.0, log6, 0))
        whole(up_out, chain_send.at[0])
        whole(dn_out, chain_send.at[1])

    @pl.when(task == 2)
    def _():
        inner(down(1.0, 2.0, 1), up(2.0, log6, 3))
        whole(up_out, chain_send.at[0])
        whole(dn_out, chain_send.at[1])

    rest = split.at[:, pl.ds(0, 7)]
    whole(rest, out_send)
    whole(out, out_recv)


def body(adjusted, fisher):
    models, rows, columns = adjusted.shape
    shape = (models, ROWS, 8, columns)
    chain = pltpu.VMEM((ROWS, 2, 8, (1 + 2 * TILES) * LANES), BF16)
    out = pl.pallas_call(
        kernel,
        out_shape=jax.ShapeDtypeStruct((8, 8, ROWS, 8, LANES), BF16),
        in_specs=[pl.BlockSpec(memory_space=pl.ANY)] * 2,
        out_specs=pl.BlockSpec(memory_space=pltpu.VMEM),
        scratch_shapes=[
            pltpu.VMEM(shape, BF16),
            pltpu.VMEM(shape, BF16),
            chain, chain, chain, chain,
            pltpu.VMEM((8, TILES * LANES), F32),
            pltpu.VMEM((ROWS, 16, 8, SEG_PAD), BF16),
            pltpu.VMEM((ROWS, 8, 8, SEG_PAD), BF16),
            pltpu.VMEM((ROWS, len(HEAD), 8, LANES), BF16),
            pltpu.VMEM((ROWS, 8, 8, LANES), BF16),
            pltpu.VMEM((ROWS, 8, 8, 8, LANES), BF16),
            pltpu.SemaphoreType.DMA((2, ROWS)),
            pltpu.SemaphoreType.DMA((2, STEPS, len(PIECES))),
            pltpu.SemaphoreType.DMA((2,)),
            pltpu.SemaphoreType.DMA((ROWS,)),
            pltpu.SemaphoreType.DMA,
            pltpu.SemaphoreType.DMA((ROWS,)),
            pltpu.SemaphoreType.DMA,
            pltpu.SemaphoreType.DMA,
            pltpu.SemaphoreType.DMA,
        ],
        compiler_params=pltpu.CompilerParams(collective_id=0, has_side_effects=True),
    )(adjusted.reshape(shape), fisher.reshape(shape))
    return out.reshape(-1, LANES)[:, :OWN]


def solution(mesh):
    return jax.shard_map(
        body,
        mesh=mesh,
        in_specs=(P("task", "tile", None), P("task", "tile", None)),
        out_specs=P(None, ("task", "tile")),
        check_vma=False,
    )
```

```python
import functools
import math

import jax
import jax.numpy as jnp
from jax import lax
from jax.experimental import pallas as pl
from jax.experimental.pallas import tpu as pltpu
from jax.sharding import PartitionSpec as P

MESH = pl.DeviceIdType.MESH
F32 = jnp.float32
BF16 = jnp.bfloat16

ROWS, TILES, LANES = 7, 37, 128
SEG, SEG_PAD, OWN = 592, 640, 74
PIECES = ((0, 10), (10, 9), (19, 9), (28, 9))
GROUP = 5
STEPS = 2 * ROWS
AHEAD, LAG, DELAY, SKEW = 5, 2, 7, 5
HELD, RELEASE, HOLD_OTHER = 5, 9, True
EVEN = (*range(0, 5), *range(9, 14), *range(18, 23), *range(28, 32))
ODD = (*range(5, 9), *range(14, 18), *range(23, 28), *range(32, 37))
HEAD = {1: 48, 3: 16, 4: 0, 6: 32}
TAIL = {1: 48, 3: 16, 4: 64, 6: 32}

Q_POWER, Q_TOP, Q_KNEE = 24.0, 120.0, -9.5
Q_FLOOR = 2.0 ** (Q_TOP + Q_POWER * Q_KNEE)
Q_LINE = Q_FLOOR / 2.0**Q_KNEE
D_POWER, D_MID = 25.0, -1.665
INV_LN2 = 1.0 / math.log(2.0)


def log2(x):
    return jnp.log(x) * INV_LN2


def encode_q(q, inverse_scale):
    y = jnp.abs(q) * inverse_scale
    knee = 2.0**Q_KNEE
    power = jnp.exp2(log2(jnp.maximum(y, knee)) * Q_POWER + Q_TOP)
    code = jnp.where(y >= knee, power, y * Q_LINE)
    return jnp.where(q < 0, -code, code).astype(BF16)


def decode_q(code, scale):
    c = code.astype(F32)
    size = jnp.abs(c)
    root = jnp.exp2((log2(jnp.maximum(size, Q_FLOOR)) - Q_TOP) * (1.0 / Q_POWER))
    y = jnp.where(size >= Q_FLOOR, root, size * (1.0 / Q_LINE)) * scale
    return jnp.where(c < 0, -y, y)


def encode_d(d, log_count):
    return jnp.exp2((log2(d) - (log_count + D_MID)) * D_POWER).astype(BF16)


def decode_d(code, log_count):
    return jnp.exp2(log2(code.astype(F32)) * (1.0 / D_POWER) + (log_count + D_MID))


def lanes(tile, count=1):
    start = tile * LANES
    return pl.ds(start if isinstance(start, int) else pl.multiple_of(start, LANES), count * LANES)


def groups(start, count):
    return [range(a, min(a + GROUP, start + count)) for a in range(start, start + count, GROUP)]


def kernel(a_hbm, f_hbm, out, av, fv, up_in, up_out, dn_in, dn_out, merged, seg_out, seg_in, edge_out, edge_in, split,
           in_sem, chain_recv, chain_send, seg_recv, seg_send, edge_recv, edge_send, out_recv, out_send):
    task, tile = lax.axis_index("task"), lax.axis_index("tile")
    slot, side = tile // 8, tile % 8

    def loads(r):
        return (pltpu.make_async_copy(a_hbm.at[:, r], av.at[:, r], in_sem.at[0, r]),
                pltpu.make_async_copy(f_hbm.at[:, r], fv.at[:, r], in_sem.at[1, r]))

    for r in range(ROWS):
        for copy in loads(r):
            copy.start()

    edge_in[...] = jnp.zeros_like(edge_in)
    barrier = pltpu.get_barrier_semaphore()
    place = task * 8 + slot

    def greet_column(i, carry):
        other = (place + i) % 32
        pl.semaphore_signal(barrier, inc=1, device_id=(other // 8, (other % 8) * 8 + side), device_id_type=MESH)
        return carry

    def greet_side(i, carry):
        pl.semaphore_signal(barrier, inc=1, device_id=(task, slot * 8 + (side + i) % 8), device_id_type=MESH)
        return carry

    lax.fori_loop(1, 32, greet_column, 0)
    lax.fori_loop(1, 8, greet_side, 0)

    def wait_rows(i):
        @pl.when(i % 2 == 0)
        def _():
            for copy in loads(i // 2):
                copy.wait()

    half = slot % 2
    odd_task = (3 * half, 3 - 3 * half)
    even_task = (3 - 3 * half, 3 * half)

    def column(i, way, x):
        if x < len(ODD):
            other = odd_task[way] * TILES + ODD[x]
        else:
            other = even_task[way] * TILES + EVEN[x - len(ODD)]
        return lanes(jnp.where(i % 2 == 0, (1 + way) * TILES + x, other))

    def own(i, way, tiles):
        r = i // 2
        n, d = [], []
        for x in tiles:
            at = column(i, way, x)
            f0, f1 = fv[0, r, :, at].astype(F32), fv[1, r, :, at].astype(F32)
            n.append(f0 * av[0, r, :, at].astype(F32) + f1 * av[1, r, :, at].astype(F32))
            d.append(f0 + f1)
        return n, d

    def own_scale(i, way):
        r = i // 2
        tops = [jnp.full((8, LANES), 2.0**-96, F32) for _ in range(4)]
        for x in range(TILES):
            at = column(i, way, x)
            for m in range(2):
                k = (2 * x + m) % 4
                tops[k] = jnp.maximum(tops[k], jnp.abs(av[m, r, :, at].astype(F32)))
        return jnp.maximum(jnp.maximum(tops[0], tops[1]), jnp.maximum(tops[2], tops[3]))

    def span(piece):
        start, count = PIECES[piece]
        low = 0 if piece == 0 else 1 + 2 * start
        return pl.ds(low * LANES, (1 + 2 * (start + count) - low) * LANES)

    def hop(i, piece, source, target, way, to):
        r, t = i // 2, i % 2
        at = span(piece)
        return pltpu.make_async_remote_copy(
            src_ref=source.at[r, t, :, at], dst_ref=target.at[r, t, :, at],
            send_sem=chain_send.at[way], recv_sem=chain_recv.at[way, i, piece],
            device_id=(to, tile), device_id_type=MESH)

    def arrived(i, piece, target, way):
        r, t = i // 2, i % 2
        at = span(piece)
        pltpu.make_async_copy(target.at[r, t, :, at], target.at[r, t, :, at], chain_recv.at[way, i, piece]).wait()

    def received(i, piece, tiles, source, log_count, scale):
        r, t = i // 2, i % 2
        start, count = PIECES[piece]
        q = [decode_q(source[r, t, :, lanes(1 + start + x)], scale) for x in tiles]
        d = [decode_d(source[r, t, :, lanes(1 + start + count + x)], log_count) for x in tiles]
        return q, d

    def put(i, piece, tiles, n, d, target, log_count, inverse):
        r, t = i // 2, i % 2
        start, count = PIECES[piece]
        q = [encode_q(a / b, inverse) for a, b in zip(n, d)]
        e = [encode_d(b, log_count) for b in d]
        for x, code in zip(tiles, q):
            target[r, t, :, lanes(1 + start + x)] = code
        for x, code in zip(tiles, e):
            target[r, t, :, lanes(1 + start + count + x)] = code

    def first(i, way, target, landing, to, send=True):
        wait_rows(i)
        scale = own_scale(i, way)
        inverse = 1.0 / scale
        target[i // 2, i % 2, :, lanes(0)] = scale.astype(BF16)
        for piece, (start, count) in enumerate(PIECES):
            for tiles in groups(start, count):
                n, d = own(i, way, tiles)
                put(i, piece, tiles, n, d, target, 1.0, inverse)
            if send:
                hop(i, piece, target, landing, way, to).start()

    def middle(i, piece, way, source, target, to, log_in, log_out):
        r, t = i // 2, i % 2
        start, count = PIECES[piece]
        if piece == 0:
            mine = own_scale(i, way)
        arrived(i, piece, source, way)
        before = source[r, t, :, lanes(0)].astype(F32)
        if piece == 0:
            scale = jnp.maximum(before, mine)
            target[r, t, :, lanes(0)] = scale.astype(BF16)
        else:
            scale = target[r, t, :, lanes(0)].astype(F32)
        inverse = 1.0 / scale
        for tiles in groups(start, count):
            n, d = own(i, way, tiles)
            q, e = received(i, piece, tiles, source, log_in, before)
            n = [x + a * b for x, a, b in zip(n, q, e)]
            d = [x + b for x, b in zip(d, e)]
            put(i, piece, tiles, n, d, target, log_out, inverse)
        hop(i, piece, target, source, way, to).start()

    lane = lax.broadcasted_iota(jnp.int32, (8, LANES), 1)

    def hand_in(r, way, z):
        def send(y, carry):
            k = 2 * y + z
            pltpu.make_async_remote_copy(
                src_ref=seg_out.at[r, k], dst_ref=seg_in.at[r, half, slot // 2],
                send_sem=seg_send, recv_sem=seg_recv.at[r, half],
                device_id=(1 + way, k * 8 + side), device_id_type=MESH).start()
            return carry

        lax.fori_loop(0, 4, send, 0)

    def last(i, way, source):
        r, t = i // 2, i % 2
        for piece, (start, count) in enumerate(PIECES):
            arrived(i, piece, source, way)
            if piece == 0:
                before = source[r, t, :, lanes(0)].astype(F32)
            for tiles in groups(start, count):
                n, d = own(i, way, tiles)
                q, e = received(i, piece, tiles, source, math.log2(6.0), before)
                for x, n1, d1, q1, e1 in zip(tiles, n, d, q, e):
                    merged[:, lanes(x)] = (n1 + q1 * e1) / (d1 + e1)

        def shift(where, k):
            part = merged[:, lanes(where)]
            return pltpu.roll(part, LANES - SEG * k % LANES, 1) if SEG * k % LANES else part

        def join(low, high, edge):
            if low is None or high is None:
                return high if low is None else low
            return jnp.where(lane < edge, low, high)

        def pack(place_of):
            for k in range(8):
                low, off = SEG * k // LANES, SEG * k % LANES
                held = [place_of(k, low + j) for j in range(6 if off else 5)]
                parts = [None if x is None else shift(x, k) for x in held]
                for j in range(5):
                    part = join(parts[j], parts[j + 1], LANES - off) if off else parts[j]
                    seg_out[r, 8 * t + k, :, lanes(j)] = part.astype(BF16)

        @pl.when(t == 0)
        def _():
            pack(lambda k, x: x if x < TILES else None)
            if not HOLD_OTHER:
                hand_in(r, way, 1 - half)

            @pl.when(r >= HELD)
            def _():
                hand_in(r, way, half)
                if HOLD_OTHER:
                    hand_in(r, way, 1 - half)

        @pl.when(t == 1)
        def _():
            def place_of(k, x):
                if k % 2:
                    return ODD.index(x) if x in ODD else None
                return len(ODD) + EVEN.index(x) if x in EVEN else None

            pack(place_of)
            for e, k in enumerate(sorted(HEAD)):
                first_tile, last_tile = SEG * k // LANES, (SEG * (k + 1) - 1) // LANES
                low = None if HEAD[k] == 0 else shift(place_of(k + 1, first_tile), k)
                edge_out[r, e] = join(low, shift(place_of(k + 1, last_tile), k), HEAD[k]).astype(BF16)
            for k in range(8):
                to = odd_task[way] if k % 2 else even_task[way]
                mine = (to == task) & (k == slot)

                @pl.when(mine)
                def _():
                    pltpu.make_async_copy(
                        seg_out.at[r, 8 + k], seg_in.at[r, half, slot // 2], seg_recv.at[r, half]).start()

                @pl.when(jnp.logical_not(mine))
                def _():
                    pltpu.make_async_remote_copy(
                        src_ref=seg_out.at[r, 8 + k], dst_ref=seg_in.at[r, half, slot // 2],
                        send_sem=seg_send, recv_sem=seg_recv.at[r, half],
                        device_id=(to, k * 8 + side), device_id_type=MESH).start()
            for e, k in enumerate(sorted(HEAD)):
                to = even_task[way] if k % 2 else odd_task[way]
                pltpu.make_async_remote_copy(
                    src_ref=edge_out.at[r, e], dst_ref=edge_in.at[r, half, slot // 2],
                    send_sem=edge_send, recv_sem=edge_recv.at[r, half],
                    device_id=(to, k * 8 + side), device_id_type=MESH).start()

    lane3 = lax.broadcasted_iota(jnp.int32, (4, 8, LANES), 2)

    shared = (task % 3 == 0) & ((slot % 5 == 1) | (slot == 3) | (slot == 4))
    head, tail = jnp.int32(0), jnp.int32(LANES)
    for k in HEAD:
        head = jnp.where(shared & (slot == k), HEAD[k], head)
        tail = jnp.where(shared & (slot == k), TAIL[k], tail)

    def spread(r, z):
        pltpu.make_async_copy(seg_in.at[r, z], seg_in.at[r, z], seg_recv.at[r, z]).wait()

        @pl.when(shared)
        def _():
            pltpu.make_async_copy(edge_in.at[r, z], edge_in.at[r, z], edge_recv.at[r, z]).wait()

        edge = edge_in[r, z].astype(F32)
        tiles = [seg_in[r, z, :, :, lanes(j)].astype(F32) for j in range(5)]
        tiles[0] = jnp.where(lane3 < head, edge, tiles[0])
        tiles[4] = jnp.where(lane3 >= tail, edge, tiles[4])
        for k in range(8):
            low, off = OWN * k // LANES, OWN * k % LANES
            part = tiles[low]
            if off:
                part = pltpu.roll(part, LANES - off, 2)
            if off + OWN > LANES:
                more = pltpu.roll(tiles[low + 1], LANES - off, 2)
                part = jnp.where(lane3 < LANES - off, part, more)
            split[r, z, k] = part.astype(BF16)
        pltpu.make_async_copy(split.at[r, z, side], out.at[:, z, side, r], out_recv).start()

        def send(i, carry):
            k = (side + i) % 8
            pltpu.make_async_remote_copy(
                src_ref=split.at[r, z, k], dst_ref=out.at[:, z, side, r],
                send_sem=out_send, recv_sem=out_recv,
                device_id=(task, slot * 8 + k), device_id_type=MESH).start()
            return carry

        lax.fori_loop(1, 8, send, 0)

    def loop(low, high, body):
        def step(i, carry):
            body(i)
            return carry

        lax.fori_loop(low, high, step, 0)

    def outer(send_way, target, landing, to, merge_way, source):
        def go(i):
            first(i, send_way, target, landing, to)

        for piece in range(len(PIECES)):
            hop(0, piece, target, landing, send_way, to).start()
        loop(1, AHEAD, go)

        def step(i):
            last(i, merge_way, source)
            for j in range(2):
                held = i - RELEASE + j

                @pl.when((held % 2 == j) & (held >= j) & (held < HELD))
                def _():
                    hand_in(held, merge_way, half)
                    if HOLD_OTHER:
                        hand_in(held, merge_way, 1 - half)

            @pl.when(i + AHEAD < STEPS)
            def _():
                go(i + AHEAD)

            @pl.when((i % 2 == 1) & (i // 2 >= LAG))
            def _():
                loop(0, 2, lambda z: spread(i // 2 - LAG, z))

        loop(0, STEPS, step)
        loop(2 * (ROWS - LAG), 2 * ROWS, lambda i: spread(i // 2, i % 2))

    def inner(lead, trail):
        def step(i):
            @pl.when(i < STEPS)
            def _():
                wait_rows(i)

            for piece in range(len(PIECES)):
                back, late = (piece - SKEW) // len(PIECES), (piece - SKEW) % len(PIECES)

                @pl.when(i < STEPS)
                def _():
                    lead(i, piece)

                @pl.when((i + back >= 0) & (i + back < STEPS))
                def _():
                    trail(i + back, late)

            @pl.when((i % 2 == 1) & (i // 2 >= DELAY))
            def _():
                spread(i // 2 - DELAY, 1 - half)

        steps = STEPS - (-SKEW // len(PIECES))
        loop(0, steps, step)
        done = steps // 2 - DELAY

        def finish(r):
            spread(r, half)

            @pl.when(r >= done)
            def _():
                spread(r, 1 - half)

        loop(0, ROWS, finish)

    log6 = math.log2(6.0)

    def up(log_in, log_out, to):
        return lambda i, piece: middle(i, piece, 0, up_in, up_out, to, log_in, log_out)

    def down(log_in, log_out, to):
        return lambda i, piece: middle(i, piece, 1, dn_in, dn_out, to, log_in, log_out)

    @pl.when(task == 0)
    def _():
        first(0, 0, up_out, up_in, 1, False)

    @pl.when(task == 3)
    def _():
        first(0, 1, dn_out, dn_in, 2, False)

    pl.semaphore_wait(barrier, 38)

    def whole(ref, sem):
        pltpu.make_async_copy(ref, ref, sem).wait()

    @pl.when(task == 0)
    def _():
        outer(0, up_out, up_in, 1, 1, dn_in)
        whole(up_out, chain_send.at[0])
        whole(seg_out.at[:, pl.ds(0, 15)], seg_send)
        whole(edge_out, edge_send)

    @pl.when(task == 3)
    def _():
        outer(1, dn_out, dn_in, 2, 0, up_in)
        whole(dn_out, chain_send.at[1])
        whole(seg_out.at[:, pl.ds(0, 15)], seg_send)
        whole(edge_out, edge_send)

    @pl.when(task == 1)
    def _():
        inner(up(1.0, 2.0, 2), down(2.0, log6, 0))
        whole(up_out, chain_send.at[0])
        whole(dn_out, chain_send.at[1])

    @pl.when(task == 2)
    def _():
        inner(down(1.0, 2.0, 1), up(2.0, log6, 3))
        whole(up_out, chain_send.at[0])
        whole(dn_out, chain_send.at[1])

    rest = split.at[:, :, pl.ds(0, 7)]
    whole(rest, out_send)
    whole(out, out_recv)


def body(adjusted, fisher):
    models, rows, columns = adjusted.shape
    shape = (models, ROWS, 8, columns)
    chain = pltpu.VMEM((ROWS, 2, 8, (1 + 2 * TILES) * LANES), BF16)
    out = pl.pallas_call(
        kernel,
        out_shape=jax.ShapeDtypeStruct((4, 2, 8, ROWS, 8, LANES), BF16),
        in_specs=[pl.BlockSpec(memory_space=pl.ANY)] * 2,
        out_specs=pl.BlockSpec(memory_space=pl.ANY),
        scratch_shapes=[
            pltpu.VMEM(shape, BF16),
            pltpu.VMEM(shape, BF16),
            chain, chain, chain, chain,
            pltpu.VMEM((8, TILES * LANES), F32),
            pltpu.VMEM((ROWS, 16, 8, SEG_PAD), BF16),
            pltpu.VMEM((ROWS, 2, 4, 8, SEG_PAD), BF16),
            pltpu.VMEM((ROWS, len(HEAD), 8, LANES), BF16),
            pltpu.VMEM((ROWS, 2, 4, 8, LANES), BF16),
            pltpu.VMEM((ROWS, 2, 8, 4, 8, LANES), BF16),
            pltpu.SemaphoreType.DMA((2, ROWS)),
            pltpu.SemaphoreType.DMA((2, STEPS, len(PIECES))),
            pltpu.SemaphoreType.DMA((2,)),
            pltpu.SemaphoreType.DMA((ROWS, 2)),
            pltpu.SemaphoreType.DMA,
            pltpu.SemaphoreType.DMA((ROWS, 2)),
            pltpu.SemaphoreType.DMA,
            pltpu.SemaphoreType.DMA,
            pltpu.SemaphoreType.DMA,
        ],
        compiler_params=pltpu.CompilerParams(collective_id=0, has_side_effects=True),
    )(adjusted.reshape(shape), fisher.reshape(shape))
    return out.reshape(-1, LANES)[:, :OWN]


def solution(mesh):
    return jax.shard_map(
        body,
        mesh=mesh,
        in_specs=(P("task", "tile", None), P("task", "tile", None)),
        out_specs=P(None, ("task", "tile")),
        check_vma=False,
    )
```

```python
import functools
import math

import jax
import jax.numpy as jnp
from jax import lax
from jax.experimental import pallas as pl
from jax.experimental.pallas import tpu as pltpu
from jax.sharding import PartitionSpec as P

MESH = pl.DeviceIdType.MESH
F32 = jnp.float32
BF16 = jnp.bfloat16

ROWS, TILES, LANES = 7, 37, 128
SEG, SEG_PAD, OWN = 592, 640, 74
PIECES = ((0, 10), (10, 9), (19, 9), (28, 9))
GROUP = 5
STEPS = 2 * ROWS
AHEAD, LAG, DELAY, SKEW = 5, 1, 7, 5
HELD, RELEASE, HOLD_OTHER = 5, 9, True
EVEN = (*range(0, 5), *range(9, 14), *range(18, 23), *range(28, 32))
ODD = (*range(5, 9), *range(14, 18), *range(23, 28), *range(32, 37))
HEAD = {1: 48, 3: 16, 4: 0, 6: 32}
TAIL = {1: 48, 3: 16, 4: 64, 6: 32}

Q_POWER, Q_TOP, Q_KNEE = 24.0, 120.0, -9.5
Q_FLOOR = 2.0 ** (Q_TOP + Q_POWER * Q_KNEE)
Q_LINE = Q_FLOOR / 2.0**Q_KNEE
D_POWER, D_MID = 25.0, -1.665
INV_LN2 = 1.0 / math.log(2.0)


def log2(x):
    return jnp.log(x) * INV_LN2


def encode_q(q, inverse_scale):
    y = jnp.abs(q) * inverse_scale
    knee = 2.0**Q_KNEE
    power = jnp.exp2(log2(jnp.maximum(y, knee)) * Q_POWER + Q_TOP)
    code = jnp.where(y >= knee, power, y * Q_LINE)
    return jnp.where(q < 0, -code, code).astype(BF16)


def decode_q(code, scale):
    c = code.astype(F32)
    size = jnp.abs(c)
    root = jnp.exp2((log2(jnp.maximum(size, Q_FLOOR)) - Q_TOP) * (1.0 / Q_POWER))
    y = jnp.where(size >= Q_FLOOR, root, size * (1.0 / Q_LINE)) * scale
    return jnp.where(c < 0, -y, y)


def encode_d(d, log_count):
    return jnp.exp2((log2(d) - (log_count + D_MID)) * D_POWER).astype(BF16)


def decode_d(code, log_count):
    return jnp.exp2(log2(code.astype(F32)) * (1.0 / D_POWER) + (log_count + D_MID))


def lanes(tile, count=1):
    start = tile * LANES
    return pl.ds(start if isinstance(start, int) else pl.multiple_of(start, LANES), count * LANES)


def groups(start, count):
    return [range(a, min(a + GROUP, start + count)) for a in range(start, start + count, GROUP)]


def kernel(a_hbm, f_hbm, out, av, fv, up_in, up_out, dn_in, dn_out, merged, seg_out, seg_in, edge_out, edge_in, split,
           in_sem, chain_recv, chain_send, seg_recv, seg_send, edge_recv, edge_send, out_recv, out_send):
    task, tile = lax.axis_index("task"), lax.axis_index("tile")
    slot, side = tile // 8, tile % 8

    def loads(r):
        return (pltpu.make_async_copy(a_hbm.at[:, r], av.at[:, r], in_sem.at[0, r]),
                pltpu.make_async_copy(f_hbm.at[:, r], fv.at[:, r], in_sem.at[1, r]))

    for r in range(ROWS):
        for copy in loads(r):
            copy.start()

    edge_in[...] = jnp.zeros_like(edge_in)
    barrier = pltpu.get_barrier_semaphore()
    place = task * 8 + slot

    def greet_column(i, carry):
        other = (place + i) % 32
        pl.semaphore_signal(barrier, inc=1, device_id=(other // 8, (other % 8) * 8 + side), device_id_type=MESH)
        return carry

    def greet_side(i, carry):
        pl.semaphore_signal(barrier, inc=1, device_id=(task, slot * 8 + (side + i) % 8), device_id_type=MESH)
        return carry

    lax.fori_loop(1, 32, greet_column, 0)
    lax.fori_loop(1, 8, greet_side, 0)

    def wait_rows(i):
        @pl.when(i % 2 == 0)
        def _():
            for copy in loads(i // 2):
                copy.wait()

    half = slot % 2
    odd_task = (3 * half, 3 - 3 * half)
    even_task = (3 - 3 * half, 3 * half)

    def column(i, way, x):
        if x < len(ODD):
            other = odd_task[way] * TILES + ODD[x]
        else:
            other = even_task[way] * TILES + EVEN[x - len(ODD)]
        return lanes(jnp.where(i % 2 == 0, (1 + way) * TILES + x, other))

    def own(i, way, tiles):
        r = i // 2
        n, d = [], []
        for x in tiles:
            at = column(i, way, x)
            f0, f1 = fv[0, r, :, at].astype(F32), fv[1, r, :, at].astype(F32)
            n.append(f0 * av[0, r, :, at].astype(F32) + f1 * av[1, r, :, at].astype(F32))
            d.append(f0 + f1)
        return n, d

    def own_scale(i, way):
        r = i // 2
        tops = [jnp.full((8, LANES), 2.0**-96, F32) for _ in range(4)]
        for x in range(TILES):
            at = column(i, way, x)
            for m in range(2):
                k = (2 * x + m) % 4
                tops[k] = jnp.maximum(tops[k], jnp.abs(av[m, r, :, at].astype(F32)))
        return jnp.maximum(jnp.maximum(tops[0], tops[1]), jnp.maximum(tops[2], tops[3]))

    def span(piece):
        start, count = PIECES[piece]
        low = 0 if piece == 0 else 1 + 2 * start
        return pl.ds(low * LANES, (1 + 2 * (start + count) - low) * LANES)

    def hop(i, piece, source, target, way, to):
        r, t = i // 2, i % 2
        at = span(piece)
        return pltpu.make_async_remote_copy(
            src_ref=source.at[r, t, :, at], dst_ref=target.at[r, t, :, at],
            send_sem=chain_send.at[way], recv_sem=chain_recv.at[way, i, piece],
            device_id=(to, tile), device_id_type=MESH)

    def arrived(i, piece, target, way):
        r, t = i // 2, i % 2
        at = span(piece)
        pltpu.make_async_copy(target.at[r, t, :, at], target.at[r, t, :, at], chain_recv.at[way, i, piece]).wait()

    def received(i, piece, tiles, source, log_count, scale):
        r, t = i // 2, i % 2
        start, count = PIECES[piece]
        q = [decode_q(source[r, t, :, lanes(1 + start + x)], scale) for x in tiles]
        d = [decode_d(source[r, t, :, lanes(1 + start + count + x)], log_count) for x in tiles]
        return q, d

    def put(i, piece, tiles, n, d, target, log_count, inverse):
        r, t = i // 2, i % 2
        start, count = PIECES[piece]
        q = [encode_q(a / b, inverse) for a, b in zip(n, d)]
        e = [encode_d(b, log_count) for b in d]
        for x, code in zip(tiles, q):
            target[r, t, :, lanes(1 + start + x)] = code
        for x, code in zip(tiles, e):
            target[r, t, :, lanes(1 + start + count + x)] = code

    def first(i, way, target, landing, to, send=True):
        wait_rows(i)
        scale = own_scale(i, way)
        inverse = 1.0 / scale
        target[i // 2, i % 2, :, lanes(0)] = scale.astype(BF16)
        for piece, (start, count) in enumerate(PIECES):
            for tiles in groups(start, count):
                n, d = own(i, way, tiles)
                put(i, piece, tiles, n, d, target, 1.0, inverse)
            if send:
                hop(i, piece, target, landing, way, to).start()

    def middle(i, piece, way, source, target, to, log_in, log_out):
        r, t = i // 2, i % 2
        start, count = PIECES[piece]
        if piece == 0:
            mine = own_scale(i, way)
        arrived(i, piece, source, way)
        before = source[r, t, :, lanes(0)].astype(F32)
        if piece == 0:
            scale = jnp.maximum(before, mine)
            target[r, t, :, lanes(0)] = scale.astype(BF16)
        else:
            scale = target[r, t, :, lanes(0)].astype(F32)
        inverse = 1.0 / scale
        for tiles in groups(start, count):
            n, d = own(i, way, tiles)
            q, e = received(i, piece, tiles, source, log_in, before)
            n = [x + a * b for x, a, b in zip(n, q, e)]
            d = [x + b for x, b in zip(d, e)]
            put(i, piece, tiles, n, d, target, log_out, inverse)
        hop(i, piece, target, source, way, to).start()

    lane = lax.broadcasted_iota(jnp.int32, (8, LANES), 1)

    def hand_in(r, way, z):
        def send(y, carry):
            k = 2 * y + z
            pltpu.make_async_remote_copy(
                src_ref=seg_out.at[r, k], dst_ref=seg_in.at[r, half, slot // 2],
                send_sem=seg_send, recv_sem=seg_recv.at[r, half],
                device_id=(1 + way, k * 8 + side), device_id_type=MESH).start()
            return carry

        lax.fori_loop(0, 4, send, 0)

    def last(i, way, source):
        r, t = i // 2, i % 2
        for piece, (start, count) in enumerate(PIECES):
            arrived(i, piece, source, way)
            if piece == 0:
                before = source[r, t, :, lanes(0)].astype(F32)
            for tiles in groups(start, count):
                n, d = own(i, way, tiles)
                q, e = received(i, piece, tiles, source, math.log2(6.0), before)
                for x, n1, d1, q1, e1 in zip(tiles, n, d, q, e):
                    merged[:, lanes(x)] = (n1 + q1 * e1) / (d1 + e1)

        def shift(where, k):
            part = merged[:, lanes(where)]
            return pltpu.roll(part, LANES - SEG * k % LANES, 1) if SEG * k % LANES else part

        def join(low, high, edge):
            if low is None or high is None:
                return high if low is None else low
            return jnp.where(lane < edge, low, high)

        def pack(place_of):
            for k in range(8):
                low, off = SEG * k // LANES, SEG * k % LANES
                held = [place_of(k, low + j) for j in range(6 if off else 5)]
                parts = [None if x is None else shift(x, k) for x in held]
                for j in range(5):
                    part = join(parts[j], parts[j + 1], LANES - off) if off else parts[j]
                    seg_out[r, 8 * t + k, :, lanes(j)] = part.astype(BF16)

        @pl.when(t == 0)
        def _():
            pack(lambda k, x: x if x < TILES else None)
            if not HOLD_OTHER:
                hand_in(r, way, 1 - half)

            @pl.when(r >= HELD)
            def _():
                hand_in(r, way, half)
                if HOLD_OTHER:
                    hand_in(r, way, 1 - half)

        @pl.when(t == 1)
        def _():
            def place_of(k, x):
                if k % 2:
                    return ODD.index(x) if x in ODD else None
                return len(ODD) + EVEN.index(x) if x in EVEN else None

            pack(place_of)
            for e, k in enumerate(sorted(HEAD)):
                first_tile, last_tile = SEG * k // LANES, (SEG * (k + 1) - 1) // LANES
                low = None if HEAD[k] == 0 else shift(place_of(k + 1, first_tile), k)
                edge_out[r, e] = join(low, shift(place_of(k + 1, last_tile), k), HEAD[k]).astype(BF16)
            for k in range(8):
                to = odd_task[way] if k % 2 else even_task[way]
                mine = (to == task) & (k == slot)

                @pl.when(mine)
                def _():
                    pltpu.make_async_copy(
                        seg_out.at[r, 8 + k], seg_in.at[r, half, slot // 2], seg_recv.at[r, half]).start()

                @pl.when(jnp.logical_not(mine))
                def _():
                    pltpu.make_async_remote_copy(
                        src_ref=seg_out.at[r, 8 + k], dst_ref=seg_in.at[r, half, slot // 2],
                        send_sem=seg_send, recv_sem=seg_recv.at[r, half],
                        device_id=(to, k * 8 + side), device_id_type=MESH).start()
            for e, k in enumerate(sorted(HEAD)):
                to = even_task[way] if k % 2 else odd_task[way]
                pltpu.make_async_remote_copy(
                    src_ref=edge_out.at[r, e], dst_ref=edge_in.at[r, half, slot // 2],
                    send_sem=edge_send, recv_sem=edge_recv.at[r, half],
                    device_id=(to, k * 8 + side), device_id_type=MESH).start()

    lane3 = lax.broadcasted_iota(jnp.int32, (4, 8, LANES), 2)

    shared = (task % 3 == 0) & ((slot % 5 == 1) | (slot == 3) | (slot == 4))
    head, tail = jnp.int32(0), jnp.int32(LANES)
    for k in HEAD:
        head = jnp.where(shared & (slot == k), HEAD[k], head)
        tail = jnp.where(shared & (slot == k), TAIL[k], tail)

    def spread(r, z):
        pltpu.make_async_copy(seg_in.at[r, z], seg_in.at[r, z], seg_recv.at[r, z]).wait()

        @pl.when(shared)
        def _():
            pltpu.make_async_copy(edge_in.at[r, z], edge_in.at[r, z], edge_recv.at[r, z]).wait()

        edge = edge_in[r, z].astype(F32)
        tiles = [seg_in[r, z, :, :, lanes(j)].astype(F32) for j in range(5)]
        tiles[0] = jnp.where(lane3 < head, edge, tiles[0])
        tiles[4] = jnp.where(lane3 >= tail, edge, tiles[4])
        for k in range(8):
            low, off = OWN * k // LANES, OWN * k % LANES
            part = tiles[low]
            if off:
                part = pltpu.roll(part, LANES - off, 2)
            if off + OWN > LANES:
                more = pltpu.roll(tiles[low + 1], LANES - off, 2)
                part = jnp.where(lane3 < LANES - off, part, more)
            split[r, z, k] = part.astype(BF16)
        pltpu.make_async_copy(split.at[r, z, side], out.at[:, z, side, r], out_recv).start()

        def send(i, carry):
            k = (side + i) % 8
            pltpu.make_async_remote_copy(
                src_ref=split.at[r, z, k], dst_ref=out.at[:, z, side, r],
                send_sem=out_send, recv_sem=out_recv,
                device_id=(task, slot * 8 + k), device_id_type=MESH).start()
            return carry

        lax.fori_loop(1, 8, send, 0)

    def loop(low, high, body):
        def step(i, carry):
            body(i)
            return carry

        lax.fori_loop(low, high, step, 0)

    def outer(send_way, target, landing, to, merge_way, source):
        def go(i):
            first(i, send_way, target, landing, to)

        for piece in range(len(PIECES)):
            hop(0, piece, target, landing, send_way, to).start()
        loop(1, AHEAD, go)

        def step(i):
            last(i, merge_way, source)
            for j in range(2):
                held = i - RELEASE + j

                @pl.when((held % 2 == j) & (held >= j) & (held < HELD))
                def _():
                    hand_in(held, merge_way, half)
                    if HOLD_OTHER:
                        hand_in(held, merge_way, 1 - half)

            @pl.when(i + AHEAD < STEPS)
            def _():
                go(i + AHEAD)

            @pl.when((i % 2 == 1) & (i // 2 >= LAG))
            def _():
                loop(0, 2, lambda z: spread(i // 2 - LAG, z))

        loop(0, STEPS, step)
        loop(2 * (ROWS - LAG), 2 * ROWS, lambda i: spread(i // 2, i % 2))

    def inner(lead, trail):
        def step(i):
            @pl.when(i < STEPS)
            def _():
                wait_rows(i)

            for piece in range(len(PIECES)):
                back, late = (piece - SKEW) // len(PIECES), (piece - SKEW) % len(PIECES)

                @pl.when(i < STEPS)
                def _():
                    lead(i, piece)

                @pl.when((i + back >= 0) & (i + back < STEPS))
                def _():
                    trail(i + back, late)

            @pl.when((i % 2 == 1) & (i // 2 >= DELAY))
            def _():
                spread(i // 2 - DELAY, 1 - half)

        steps = STEPS - (-SKEW // len(PIECES))
        loop(0, steps, step)
        done = steps // 2 - DELAY

        def finish(r):
            spread(r, half)

            @pl.when(r >= done)
            def _():
                spread(r, 1 - half)

        loop(0, ROWS, finish)

    log6 = math.log2(6.0)

    def up(log_in, log_out, to):
        return lambda i, piece: middle(i, piece, 0, up_in, up_out, to, log_in, log_out)

    def down(log_in, log_out, to):
        return lambda i, piece: middle(i, piece, 1, dn_in, dn_out, to, log_in, log_out)

    @pl.when(task == 0)
    def _():
        first(0, 0, up_out, up_in, 1, False)

    @pl.when(task == 3)
    def _():
        first(0, 1, dn_out, dn_in, 2, False)

    pl.semaphore_wait(barrier, 38)

    def whole(ref, sem):
        pltpu.make_async_copy(ref, ref, sem).wait()

    @pl.when(task == 0)
    def _():
        outer(0, up_out, up_in, 1, 1, dn_in)
        whole(up_out, chain_send.at[0])
        whole(seg_out.at[:, pl.ds(0, 15)], seg_send)
        whole(edge_out, edge_send)

    @pl.when(task == 3)
    def _():
        outer(1, dn_out, dn_in, 2, 0, up_in)
        whole(dn_out, chain_send.at[1])
        whole(seg_out.at[:, pl.ds(0, 15)], seg_send)
        whole(edge_out, edge_send)

    @pl.when(task == 1)
    def _():
        inner(up(1.0, 2.0, 2), down(2.0, log6, 0))
        whole(up_out, chain_send.at[0])
        whole(dn_out, chain_send.at[1])

    @pl.when(task == 2)
    def _():
        inner(down(1.0, 2.0, 1), up(2.0, log6, 3))
        whole(up_out, chain_send.at[0])
        whole(dn_out, chain_send.at[1])

    rest = split.at[:, :, pl.ds(0, 7)]
    whole(rest, out_send)
    whole(out, out_recv)


def body(adjusted, fisher):
    models, rows, columns = adjusted.shape
    shape = (models, ROWS, 8, columns)
    chain = pltpu.VMEM((ROWS, 2, 8, (1 + 2 * TILES) * LANES), BF16)
    out = pl.pallas_call(
        kernel,
        out_shape=jax.ShapeDtypeStruct((4, 2, 8, ROWS, 8, LANES), BF16),
        in_specs=[pl.BlockSpec(memory_space=pl.ANY)] * 2,
        out_specs=pl.BlockSpec(memory_space=pl.ANY),
        scratch_shapes=[
            pltpu.VMEM(shape, BF16),
            pltpu.VMEM(shape, BF16),
            chain, chain, chain, chain,
            pltpu.VMEM((8, TILES * LANES), F32),
            pltpu.VMEM((ROWS, 16, 8, SEG_PAD), BF16),
            pltpu.VMEM((ROWS, 2, 4, 8, SEG_PAD), BF16),
            pltpu.VMEM((ROWS, len(HEAD), 8, LANES), BF16),
            pltpu.VMEM((ROWS, 2, 4, 8, LANES), BF16),
            pltpu.VMEM((ROWS, 2, 8, 4, 8, LANES), BF16),
            pltpu.SemaphoreType.DMA((2, ROWS)),
            pltpu.SemaphoreType.DMA((2, STEPS, len(PIECES))),
            pltpu.SemaphoreType.DMA((2,)),
            pltpu.SemaphoreType.DMA((ROWS, 2)),
            pltpu.SemaphoreType.DMA,
            pltpu.SemaphoreType.DMA((ROWS, 2)),
            pltpu.SemaphoreType.DMA,
            pltpu.SemaphoreType.DMA,
            pltpu.SemaphoreType.DMA,
        ],
        compiler_params=pltpu.CompilerParams(collective_id=0, has_side_effects=True),
    )(adjusted.reshape(shape), fisher.reshape(shape))
    return out.reshape(-1, LANES)[:, :OWN]


def solution(mesh):
    return jax.shard_map(
        body,
        mesh=mesh,
        in_specs=(P("task", "tile", None), P("task", "tile", None)),
        out_specs=P(None, ("task", "tile")),
        check_vma=False,
    )
```
